32 devices in a mesh: row: 8 (over z, core), col: 4 (over y, x).
Axes of the slice: x: 2, y: 2, z: 4, core: 2. Of those that a mesh axis runs over, the one named last changes fastest.
Arguments:
- tokens: bfloat16 [512, 4096], P(None, 'col'), may hold values from -6 to 6
- w_gate: bfloat16 [4096, 10240], P('col', 'row'), may hold values from -0.09375 to 0.09375
- w_up: bfloat16 [4096, 10240], P('col', 'row'), may hold values from -0.09375 to 0.09375
- w_down: bfloat16 [10240, 4096], P('row', 'col'), may hold values from -0.0625 to 0.0625
Outputs:
- result: bfloat16 [512, 4096], P('row', 'col')
The draws below stay inside these ranges and needn't reach their ends.
All inputs are finite; a program needn't handle non-finite values.
Results may differ from the reference program's by a relative error of at most 0.025.
Values may be sent and summed in bfloat16 or wider, within the bound.
No kernel may reach another device: no remote copies, remote signals or barrier semaphores. Data moves between devices by JAX's collectives and lax.ppermute only.
A program may use at most 64 MiB of HBM per device.

```python
import jax
import jax.numpy as jnp
from jax import lax

D = 4096
FF = 10240
TOKENS = 512
N_COL = 4


def block_levels(stream_key, extent, cuts, low, largest):
    def one(dim, shards_of):
        heights = jax.random.uniform(jax.random.fold_in(jax.random.fold_in(stream_key, 6), dim), (shards_of,), jnp.float32, low / len(cuts), largest / len(cuts))
        return jnp.repeat(jnp.exp(heights), extent[dim] // shards_of).reshape((-1,) + (1,) * (len(extent) - dim - 1))

    factor_of = one(*cuts[0])
    for cut in cuts[1:]:
        factor_of = factor_of * one(*cut)
    return factor_of


def gaussian(rng, dims, scale, reach, split=(), kind=jnp.bfloat16):
    gain = block_levels(rng, dims, split, -0.22, 0.18) if split else 1.0
    array = jax.random.normal(rng, dims, jnp.float32) * scale * gain
    return jnp.minimum(jnp.maximum(array, -reach), reach).astype(kind)


def setup_inputs(seed: int = 0) -> dict:
    key_of = jax.random.split(jax.random.key(seed), 5)
    return {
        "tokens": gaussian(key_of[0], (TOKENS, D), 1.0, 6.0, ((1, 4),)),
        "w_gate": gaussian(key_of[1], (D, FF), D ** -0.5, 0.09375, ((0, 4), (1, 8))),
        "w_up": gaussian(key_of[2], (D, FF), D ** -0.5, 0.09375, ((0, 4), (1, 8))),
        "w_down": gaussian(key_of[3], (FF, D), FF ** -0.5, 0.0625, ((0, 8), (1, 4))),
    }


def reference(tokens, w_gate, w_up, w_down):
    block_width = tokens.shape[1] // N_COL
    joined = jnp.concatenate([w_gate, w_up], axis=1)
    hidden_width = w_gate.shape[1]

    def accumulate(running, block_index):
        offset = (block_index * block_width).astype(jnp.int32)
        token_rows = lax.dynamic_slice_in_dim(tokens, offset, block_width, 1)
        weight_rows = lax.dynamic_slice_in_dim(joined, offset, block_width, 0)
        product = jnp.dot(token_rows, weight_rows, preferred_element_type=jnp.float32)
        rounded = lax.optimization_barrier(product.astype(jnp.bfloat16))
        return running + rounded.astype(jnp.float32), None

    initial = jnp.zeros((tokens.shape[0], 2 * hidden_width), jnp.float32)
    summed, _ = lax.scan(accumulate, initial, jnp.arange(N_COL, dtype=jnp.int32))
    pre_gate = summed[:, :hidden_width]
    pre_up = summed[:, hidden_width:]
    hidden = (jax.nn.gelu(pre_gate, approximate=True) * pre_up).astype(jnp.bfloat16)
    return jnp.dot(hidden, w_down, preferred_element_type=jnp.float32).astype(jnp.bfloat16)
```

```python
import jax
import jax.numpy as jnp
from jax import lax
from jax.sharding import PartitionSpec as P

WAVES = 2


def pick(array, index, axis):
    return lax.dynamic_index_in_dim(array, index, axis, keepdims=False)


def wide(array):
    return array.astype(jnp.float32)


def narrow(array):
    return array.astype(jnp.bfloat16)


def activate(summed):
    return narrow(jax.nn.gelu(summed[0], approximate=True) * summed[1])


def solution(mesh):
    n_row, n_col = mesh.shape["row"], mesh.shape["col"]
    n_bits = n_col.bit_length() - 1
    colours = min(n_bits, 2)

    def swap(array, axis, distance):
        return lax.ppermute(array, axis, [(i, i ^ distance) for i in range(mesh.shape[axis])])

    def local(tokens, w_gate, w_up, w_down):
        total, depth = tokens.shape
        width = w_gate.shape[1]
        col, row = lax.axis_index("col"), lax.axis_index("row")
        core, chip = row & 1, lax.shift_right_logical(row, 1)
        own = [lax.shift_right_logical(col, b) & 1 for b in range(n_bits)]
        blocks = n_col // 2
        x = tokens.reshape(n_row, WAVES * colours * 2, -1, depth)
        unit = x.shape[2] * 2 // blocks

        def products(parts):
            together = jnp.concatenate([p.reshape(-1, depth) for p in parts])
            pair = [
                narrow(jnp.dot(together, w, preferred_element_type=jnp.float32)).reshape(len(parts), 1, n_row, -1, width)
                for w in (w_gate, w_up)
            ]
            both = lax.optimization_barrier(jnp.concatenate(pair, axis=1))
            return [both[i] for i in range(len(parts))]

        def order(c):
            return [(c + i) % n_bits for i in range(n_bits)]

        def part(w, c, bit):
            return pick(x, (w * colours + c) * 2 + bit, 1)

        sent = [products([part(w, c, 1 - own[c]) for c in range(colours)]) for w in range(WAVES)]
        kept = [products([part(w, c, own[c]) for c in range(colours)]) for w in range(WAVES)]
        got = [[swap(sent[w][c], "col", 1 << c) for c in range(colours)] for w in range(WAVES)]

        finished = []
        for w in range(WAVES):
            gathered = []
            for c in range(colours):
                bits = order(c)
                held = narrow(wide(kept[w][c]) + wide(got[w][c]))
                held = held.reshape(2, n_row, blocks // 2 if blocks > 1 else 1, -1, width)
                held = kept_sum(held, bits, own, swap)
                other = swap(held, "col", 1 << bits[-1]) if n_bits > 1 else None
                hidden = activate(wide(held) + wide(other))
                for b in reversed(bits[:-1]):
                    theirs = swap(hidden, "col", 1 << b)
                    low = jnp.where(own[b] == 0, hidden, theirs)
                    high = jnp.where(own[b] == 0, theirs, hidden)
                    hidden = jnp.concatenate([low, high], axis=1)
                gathered.append(hidden.reshape(n_row, -1, width))
            hidden = jnp.concatenate(gathered, axis=1)
            span = hidden.shape[1]
            partial = jnp.dot(hidden.reshape(-1, width), w_down, preferred_element_type=jnp.float32)
            partial = partial.reshape(n_row // 2, 2, span, -1)
            chip_sum = pick(partial, core, 1) + wide(swap(narrow(pick(partial, 1 - core, 1)), "row", 1))
            result = pick(chip_sum, chip, 0)
            for d in reversed(range(1, n_row // 2)):
                result = result + wide(swap(narrow(pick(chip_sum, chip ^ d, 0)), "row", 2 * d))
            finished.append(narrow(result))
        return jnp.concatenate(finished)

    in_specs = (P(None, "col"), P("col", "row"), P("col", "row"), P("row", "col"))
    return jax.shard_map(local, mesh=mesh, in_specs=in_specs, out_specs=P("row", "col"), check_vma=False)


def kept_sum(held, bits, own, swap):
    for b in bits[1:-1]:
        halves = held.reshape(2, held.shape[1], 2, held.shape[2] // 2, *held.shape[3:])
        theirs = swap(pick(halves, 1 - own[b], 2), "col", 1 << b)
        held = narrow(wide(pick(halves, own[b], 2)) + wide(theirs))
    return held
```

```python
import jax
import jax.numpy as jnp
from jax import lax
from jax.sharding import PartitionSpec as P

WAVES = 2


def pick(array, index, axis):
    return lax.dynamic_index_in_dim(array, index, axis, keepdims=False, allow_negative_indices=False)


def wide(array):
    return array.astype(jnp.float32)


def narrow(array):
    return array.astype(jnp.bfloat16)


def activate(summed):
    return narrow(jax.nn.gelu(summed[0], approximate=True) * summed[1])


def solution(mesh):
    n_row, n_col = mesh.shape["row"], mesh.shape["col"]
    n_bits = n_col.bit_length() - 1
    colours = min(n_bits, 2)

    def swap(array, axis, distance):
        return lax.ppermute(array, axis, [(i, i ^ distance) for i in range(mesh.shape[axis])])

    def local(tokens, w_gate, w_up, w_down):
        total, depth = tokens.shape
        width = w_gate.shape[1]
        blocks = n_col // 2
        col, row = lax.axis_index("col"), lax.axis_index("row")
        own = [lax.shift_right_logical(col, b) & 1 for b in range(n_bits)]
        away = [1 - o for o in own]
        first = [o == 0 for o in own]
        core, chip = row & 1, lax.shift_right_logical(row, 1)
        chips = [chip ^ d for d in range(n_row // 2)]
        parts = [[[(w * colours + c) * 2 + bit[c] for bit in (own, away)] for c in range(colours)] for w in range(WAVES)]
        tokens, own, away, first, core, other_core, chips, parts = lax.optimization_barrier(
            (tokens, own, away, first, core, 1 - core, chips, parts)
        )
        x = tokens.reshape(n_row, WAVES * colours * 2, -1, depth)

        def products(indices):
            together = jnp.concatenate([pick(x, i, 1).reshape(-1, depth) for i in indices])
            pair = [
                narrow(jnp.dot(together, w, preferred_element_type=jnp.float32)).reshape(len(indices), 1, n_row, -1, width)
                for w in (w_gate, w_up)
            ]
            both = jnp.concatenate(pair, axis=1)
            return [both[i] for i in range(len(indices))]

        sent = [products([parts[w][c][1] for c in range(colours)]) for w in range(WAVES)]
        kept = [products([parts[w][c][0] for c in range(colours)]) for w in range(WAVES)]
        got = [[swap(sent[w][c], "col", 1 << c) for c in range(colours)] for w in range(WAVES)]

        chip_sums = []
        for w in range(WAVES):
            gathered = []
            for c in range(colours):
                bits = [(c + i) % n_bits for i in range(n_bits)]
                held = narrow(wide(kept[w][c]) + wide(got[w][c])).reshape(2, n_row, max(blocks // 2, 1), -1, width)
                for b in bits[1:-1]:
                    halves = held.reshape(2, n_row, 2, held.shape[2] // 2, -1, width)
                    theirs = swap(pick(halves, away[b], 2), "col", 1 << b)
                    held = narrow(wide(pick(halves, own[b], 2)) + wide(theirs))
                hidden = activate(wide(held) + wide(swap(held, "col", 1 << bits[-1])))
                for b in reversed(bits[:-1]):
                    theirs = swap(hidden, "col", 1 << b)
                    low = jnp.where(first[b], hidden, theirs)
                    high = jnp.where(first[b], theirs, hidden)
                    hidden = jnp.concatenate([low, high], axis=1)
                gathered.append(hidden.reshape(n_row, -1, width))
            hidden = jnp.concatenate(gathered, axis=1)
            partial = jnp.dot(hidden.reshape(-1, width), w_down, preferred_element_type=jnp.float32)
            partial = partial.reshape(n_row // 2, 2, hidden.shape[1], -1)
            chip_sums.append(pick(partial, core, 1) + wide(swap(narrow(pick(partial, other_core, 1)), "row", 1)))
        finished = []
        for s in chip_sums:
            result = pick(s, chips[0], 0)
            for d in reversed(range(1, n_row // 2)):
                result = result + wide(swap(narrow(pick(s, chips[d], 0)), "row", 2 * d))
            finished.append(narrow(result))
        return jnp.concatenate(finished)

    in_specs = (P(None, "col"), P("col", "row"), P("col", "row"), P("row", "col"))
    return jax.shard_map(local, mesh=mesh, in_specs=in_specs, out_specs=P("row", "col"), check_vma=False)
```
